32 devices in a mesh: groups: 2 (over y), az: 4 (over z), rg: 2 (over x), acq: 2 (over core).
Axes of the slice: x: 2, y: 2, z: 4, core: 2. Of those that a mesh axis runs over, the one named last changes fastest.
Arguments:
- image_stack: bfloat16 [2, 64, 32, 4, 256], P(None, ('az', 'acq'), 'groups', 'rg'), parts along dimension 2, may hold values from -12 to 12
- steering: bfloat16 [4, 2, 64, 512], P('rg'), as said below
- wiener_filter: bfloat16 [4, 2, 64, 64], P('rg'), may hold values from -0.5 to 0.5
- range_group: int32 [4], P('rg'), may hold values from 0 to 3, as said below
- lay_list: int32 [32, 4, 32], P(('groups', 'az', 'acq'), 'rg'), parts along dimension 0, may hold values from 0 to 255, as said below
- lay_count: int32 [32, 4], P(('groups', 'az', 'acq'), 'rg'), parts along dimension 0, may hold values from 0 to 32, as said below
Outputs:
- power: bfloat16 [32, 4, 512, 256], P(('groups', 'az', 'acq'), 'rg'), parts along dimension 0
The draws below stay inside these ranges and needn't reach their ends.
There are 2 independent parts, one for each index of `groups`. The reference program is written for one: setup_inputs(seed, part) draws one part's arguments, and reference() takes and returns one part's arrays. A program takes and returns all parts, laid end to end along the dimension named above; an argument that names none is the same for every part. Nothing has to cross between parts.
Inputs may be any that keep to these rules, and one draw needn't show every extreme that they name: `lay_list`: within one block the 32 entries are distinct pixels. The first lay_count entries of a block's list are its layover pixels; some block has 32. `range_group`: range block r belongs to a group from (r // 2) * 2 to (r // 2) * 2 + 1. `steering`: every complex entry has modulus 1 / sqrt(512) up to rounding.
All inputs are finite; a program needn't handle non-finite values.
Results may differ from the reference program's by a relative error of at most 0.0075.
Values may be sent and summed in bfloat16 or wider, within the bound.
A program may use at most 64 MiB of HBM per device.

```python
import math
import jax
import jax.numpy as jnp
from jax import lax

K = 64
E = 512
BLK = 256
LMAX = 32
GRP_DEV = 2
ITERS = 8
AZB_DEV = 2
RGB_DEV = 2
AZB = 16
RGB = 4
NGRP = 4


def draw_steering(key, part):
    phases = jax.random.uniform(key, (NGRP, K, E), jnp.float32, -math.pi, math.pi)
    scale = 1.0 / math.sqrt(E)
    return (jnp.stack([jnp.cos(phases), jnp.sin(phases)], axis=1) * scale).astype(jnp.bfloat16)


def draw_range_group(key, part):
    wide_values = jax.random.randint(key, (RGB,), 0, 1048576, dtype=jnp.int32)
    offset = wide_values % GRP_DEV
    return jnp.arange(RGB, dtype=jnp.int32) // RGB_DEV * GRP_DEV + offset


def draw_lay_list(key, part):
    scores = jax.random.randint(jax.random.fold_in(key, 21), (AZB, RGB, BLK), 0, 1048576, dtype=jnp.int32)
    scores = scores * BLK + jnp.arange(BLK, dtype=jnp.int32)
    ordering = jnp.argsort(scores, axis=-1)
    return ordering[:, :, :LMAX].astype(jnp.int32)


def draw_lay_count(key, part):
    urban_flag = jax.random.randint(jax.random.fold_in(key, 31), (AZB // AZB_DEV, RGB // RGB_DEV), 0, 4, dtype=jnp.int32) == 0
    urban_flag = jnp.repeat(jnp.repeat(urban_flag, AZB_DEV, axis=0), RGB_DEV, axis=1)
    heavy_count = jax.random.randint(jax.random.fold_in(key, 32), (AZB, RGB), LMAX // 2, LMAX + 1, dtype=jnp.int32)
    light_count = jax.random.randint(jax.random.fold_in(key, 33), (AZB, RGB), 0, LMAX // 8 + 1, dtype=jnp.int32)
    counts = jnp.where(urban_flag, heavy_count, light_count)
    return counts.at[0, 0].set(LMAX)


def block_levels(key, extent, shards, smallest, high):
    level, own = 1.0, jax.random.fold_in(key, 6)
    for axis_at, shards_of in shards:
        heights = jnp.exp(jax.random.uniform(jax.random.fold_in(own, axis_at), (shards_of,), jnp.float32, smallest / len(shards), high / len(shards)))
        level = level * jnp.repeat(heights, extent[axis_at] // shards_of).reshape([-1 if axis == axis_at else 1 for axis in range(len(extent))])
    return level


def gaussian(rng, extent, spread, reach, shards=(), kind=jnp.bfloat16):
    entries = spread * jax.random.normal(rng, extent, jnp.float32)
    if shards:
        entries = entries * block_levels(rng, extent, shards, -0.22, 0.18)
    return jnp.clip(entries, -reach, reach).astype(kind)


def setup_inputs(seed: int = 0, part: int = 0) -> dict:
    splits = jax.random.split(jax.random.key(seed), 7)
    part_keys = jax.random.split(jax.random.fold_in(splits[6], part), 7)
    return {
        "image_stack": gaussian(part_keys[0], (2, K, AZB, RGB, BLK), 2.0, 12.0, ((1, 8), (3, 2))),
        "steering": draw_steering(jax.random.fold_in(splits[6], 71), part),
        "wiener_filter": gaussian(splits[2], (NGRP, 2, K, K), (2 * K) ** -0.5, 0.5, ((0, 2),)),
        "range_group": draw_range_group(jax.random.fold_in(splits[6], 71), part),
        "lay_list": draw_lay_list(jax.random.fold_in(jax.random.fold_in(splits[6], part), 71), part),
        "lay_count": draw_lay_count(jax.random.fold_in(jax.random.fold_in(splits[6], part), 71), part),
    }


STEP_SIZE = 0.5
SHRINK = 0.25

def complex_block(complex_parts):
    real_part = complex_parts[0]
    imag_part = complex_parts[1]
    upper = jnp.concatenate([real_part, -imag_part], axis=1)
    lower = jnp.concatenate([imag_part, real_part], axis=1)
    return jnp.concatenate([upper, lower], axis=0)

def ista_power(lane_data, operator):
    target = lane_data.astype(jnp.float32)
    elevation = operator.shape[1] // 2

    def sweep(sweep_index, estimate):
        rounded = estimate.astype(jnp.bfloat16)
        predicted = jnp.dot(rounded, operator.T, preferred_element_type=jnp.float32)
        misfit = (target - predicted).astype(jnp.bfloat16)
        update = estimate + STEP_SIZE * jnp.dot(misfit, operator, preferred_element_type=jnp.float32)
        magnitude = update[:, :elevation] ** 2 + update[:, elevation:] ** 2
        factor = jnp.maximum(1.0 - SHRINK * lax.rsqrt(jnp.maximum(magnitude, SHRINK * SHRINK)), 0.0)
        return update * jnp.concatenate([factor, factor], axis=1)
    start = jnp.zeros((lane_data.shape[0], 2 * elevation), jnp.float32)
    estimate = lax.fori_loop(0, ITERS, sweep, start)
    return (estimate[:, :elevation] ** 2 + estimate[:, elevation:] ** 2).astype(jnp.bfloat16)

def reference(image_stack, steering, wiener_filter, range_group, lay_list, lay_count):

    def column_power(column):
        group_id = range_group[column]
        operator = complex_block(lax.dynamic_index_in_dim(steering, group_id, 0, keepdims=False))
        filter_matrix = complex_block(lax.dynamic_index_in_dim(wiener_filter, group_id, 0, keepdims=False))
        block_data = lax.dynamic_index_in_dim(image_stack, column, 3, keepdims=False).reshape(2 * K, AZB, BLK)
        filtered = jnp.einsum('ij,jap->iap', filter_matrix.astype(jnp.float32), block_data.astype(jnp.float32)).astype(jnp.bfloat16)
        beamed = jnp.einsum('ie,iap->aep', operator.astype(jnp.float32), filtered.astype(jnp.float32))
        wiener_power = beamed[:, :E] ** 2 + beamed[:, E:] ** 2
        listed = lax.dynamic_index_in_dim(lay_list, column, 1, keepdims=False)
        live_count = lax.dynamic_index_in_dim(lay_count, column, 1, keepdims=False)
        usable = jnp.arange(LMAX, dtype=jnp.int32)[None, :] < live_count[:, None]
        chosen = ((listed[:, :, None] == jnp.arange(BLK, dtype=jnp.int32)[None, None, :]) & usable[:, :, None]).astype(jnp.float32)
        lane_data = jnp.einsum('alp,iap->ali', chosen, block_data.astype(jnp.float32)).astype(jnp.bfloat16).reshape(AZB * LMAX, 2 * K)
        lay_power = ista_power(lane_data, operator).reshape(AZB, LMAX, E)
        placed = jnp.einsum('alp,ale->aep', chosen, lay_power.astype(jnp.float32))
        covered = lax.optimization_barrier(jnp.sum(chosen, axis=1))
        return jnp.where(covered[:, None, :] > 0.5, placed, wiener_power).astype(jnp.bfloat16)
    columns = lax.map(column_power, jnp.arange(RGB, dtype=jnp.int32))
    return jnp.transpose(columns, (1, 0, 2, 3))
```

```python
import functools

import jax
import jax.numpy as jnp
from jax import lax
from jax.experimental import pallas as pl
from jax.experimental.pallas import tpu as pltpu
from jax.sharding import PartitionSpec as P

ITERS = 8
STEP_SIZE = 0.5
SHRINK = 0.25
LANES = 128
VMEM_LIMIT = 16 * 1024 * 1024
MESH = pl.DeviceIdType.MESH


def iota(shape, axis):
    return lax.broadcasted_iota(jnp.int32, shape, axis)


def exchange_kernel(
    n_az,
    n_acq,
    range_group_in,
    lay_count_in,
    image,
    steering_in,
    wiener_filter_in,
    lay_list_in,
    recv,
    op,
    op_t,
    mix,
    chosen,
    lane_mask,
    covered,
    gather,
    range_group,
    lay_count,
    steering,
    wiener_filter,
    lay_list,
    send_sem,
    recv_sem,
    local_sem,
):
    n = n_az * n_acq
    me = lax.axis_index("az") * n_acq + lax.axis_index("acq")
    halves, share, azb_all, ranges, pixels = image.shape
    blocks = azb_all // n
    groups, _, acqs, elevation = steering.shape
    rows = halves * acqs
    wide = ranges * rows
    listed = lay_list.shape[2]
    lanes = blocks * ranges * listed
    sets = blocks * ranges
    spread = rows * sets
    chunks = elevation // LANES
    bf16 = jnp.bfloat16
    f32 = jnp.float32

    def peer(index):
        return {"az": index // n_acq, "acq": lax.rem(index, n_acq)}

    barrier = pltpu.get_barrier_semaphore()
    for offset in range(1, n):
        pl.semaphore_signal(
            barrier, inc=1, device_id=peer(lax.rem(me + offset, n)), device_id_type=MESH
        )
    inputs = []
    for at, (source, target) in enumerate(
        (
            (range_group_in, range_group),
            (lay_count_in, lay_count),
            (steering_in, steering),
            (wiener_filter_in, wiener_filter),
            (lay_list_in, lay_list),
        )
    ):
        copy = pltpu.make_async_copy(source, target, local_sem.at[at + 1])
        copy.start()
        inputs.append(copy)
    local = pltpu.make_async_copy(
        image.at[:, :, pl.ds(blocks * me, blocks)],
        recv.at[:, pl.ds(share * me, share)],
        local_sem.at[0],
    )
    local.start()

    pl.semaphore_wait(barrier, n - 1)
    copies = []
    for offset in range(1, n):
        there = lax.rem(me + offset, n)
        copy = pltpu.make_async_remote_copy(
            src_ref=image.at[:, :, pl.ds(blocks * there, blocks)],
            dst_ref=recv.at[:, pl.ds(share * me, share)],
            send_sem=send_sem.at[offset],
            recv_sem=recv_sem.at[offset],
            device_id=peer(there),
            device_id_type=MESH,
        )
        copy.start()
        copies.append(copy)

    first_group = lax.axis_index("rg") * groups
    copy_rows = (iota((rows, spread), 1) // sets == iota((rows, spread), 0)).astype(bf16)
    at_row, at_column = iota((spread, wide), 0), iota((spread, wide), 1)
    gather[...] = (
        (at_row // sets == lax.rem(at_column, rows))
        & (lax.rem(at_row, ranges) == at_column // rows)
    ).astype(bf16)
    lane_range = lax.rem(iota((lanes, wide), 0) // listed, ranges)
    lane_mask[...] = jnp.where(lane_range == iota((lanes, wide), 1) // rows, STEP_SIZE, 0.0)
    for copy in inputs:
        copy.wait()
    for r in range(ranges):
        group = range_group[r] - first_group
        steer = steering[0]
        filt = wiener_filter[0]
        for g in range(1, groups):
            steer = jnp.where(group == g, steering[g], steer)
            filt = jnp.where(group == g, wiener_filter[g], filt)
        re, im = steer[0], steer[1]
        top = r * rows
        for j in range(chunks):
            cut = slice(j * LANES, (j + 1) * LANES)
            left = slice(2 * j * LANES, (2 * j + 1) * LANES)
            right = slice((2 * j + 1) * LANES, (2 * j + 2) * LANES)
            op[top : top + acqs, left] = re[:, cut]
            op[top : top + acqs, right] = -im[:, cut]
            op[top + acqs : top + rows, left] = im[:, cut]
            op[top + acqs : top + rows, right] = re[:, cut]
        upper = jnp.concatenate([filt[0], -filt[1]], axis=1)
        lower = jnp.concatenate([filt[1], filt[0]], axis=1)
        filter_matrix = jnp.concatenate([upper, lower], axis=0)
        repeated = jnp.dot(filter_matrix, copy_rows, preferred_element_type=f32)
        for b in range(blocks):
            keep = lax.rem(iota((rows, spread), 1), sets) == b * ranges + r
            at = (b * ranges + r) * rows
            mix[at : at + rows, :] = jnp.where(keep, repeated, 0.0).astype(bf16)
    for j in range(2 * chunks):
        op_t[j * LANES : (j + 1) * LANES, :] = op[:, j * LANES : (j + 1) * LANES].T

    diagonal = iota((listed, listed), 0) == iota((listed, listed), 1)
    for b in range(blocks):
        for r in range(ranges):
            entries = lay_list[b, r : r + 1, :].astype(f32)
            column = jnp.sum(jnp.where(diagonal, entries, 0.0), axis=1, keepdims=True)
            alive = iota((listed, pixels), 0) < lay_count[b, r]
            hit = (iota((listed, pixels), 1).astype(f32) == column) & alive
            hot = jnp.where(hit, 1.0, 0.0)
            at = b * ranges + r
            chosen[at * listed : (at + 1) * listed, :] = hot.astype(bf16)
            covered[at : at + 1, :] = jnp.sum(hot, axis=0, keepdims=True)

    local.wait()
    for copy in copies:
        copy.wait()


def solve_kernel(
    ranges,
    recv,
    op,
    op_t,
    mix,
    chosen,
    lane_mask,
    covered,
    gather,
    power,
    estimate,
    rounded,
    beams,
    result,
    out_sem,
):
    spread = mix.shape[0]
    wide = op.shape[0]
    rows = wide // ranges
    sets = spread // rows
    chunks = op.shape[1] // (2 * LANES)
    lanes, pixels = chosen.shape
    listed = lanes // sets
    bf16 = jnp.bfloat16
    f32 = jnp.float32

    data = recv[...].reshape(spread, pixels)
    picked = lax.dot_general(
        chosen[...], data, (((1,), (1,)), ((), ())), preferred_element_type=f32
    )
    own = iota((lanes, spread), 0) // listed == lax.rem(iota((lanes, spread), 1), sets)
    target = jnp.dot(
        jnp.where(own, picked, 0.0).astype(bf16), gather[...], preferred_element_type=f32
    )
    filtered = [
        jnp.dot(
            mix[which * rows : (which + 1) * rows, :], data, preferred_element_type=f32
        ).astype(bf16)
        for which in range(sets)
    ]

    def beam_unit(unit):
        which, j = divmod(unit, chunks)
        r = which % ranges
        beam = jnp.dot(
            op_t[2 * j * LANES : (2 * j + 2) * LANES, r * rows : (r + 1) * rows],
            filtered[which],
            preferred_element_type=f32,
        )
        re, im = beam[:LANES], beam[LANES:]
        beams[which, j * LANES : (j + 1) * LANES, :] = (re * re + im * im).astype(bf16)

    units = list(range(sets * chunks))
    turns = ITERS * chunks
    done = 0
    for turn in range(ITERS):
        if turn == 0:
            misfit = (target * STEP_SIZE).astype(bf16)
        else:
            predicted = jnp.dot(rounded[...], op_t[...], preferred_element_type=f32)
            misfit = ((target - predicted) * lane_mask[...]).astype(bf16)
        for j in range(chunks):
            left = slice(2 * j * LANES, (2 * j + 1) * LANES)
            right = slice((2 * j + 1) * LANES, (2 * j + 2) * LANES)
            both = slice(2 * j * LANES, (2 * j + 2) * LANES)
            step = jnp.dot(misfit, op[:, both], preferred_element_type=f32)
            z_re, z_im = step[:, :LANES], step[:, LANES:]
            if turn > 0:
                z_re = z_re + estimate[:, left]
                z_im = z_im + estimate[:, right]
            magnitude = z_re * z_re + z_im * z_im
            factor = jnp.maximum(
                1.0 - SHRINK * lax.rsqrt(jnp.maximum(magnitude, SHRINK * SHRINK)), 0.0
            )
            x_re, x_im = z_re * factor, z_im * factor
            if turn < ITERS - 1:
                estimate[:, left] = x_re
                estimate[:, right] = x_im
                rounded[:, left] = x_re.astype(bf16)
                rounded[:, right] = x_im.astype(bf16)
            else:
                rounded[:, j * LANES : (j + 1) * LANES] = (x_re * x_re + x_im * x_im).astype(bf16)
            due = (turn * chunks + j + 1) * len(units) // turns
            while done < due:
                beam_unit(units[done])
                done += 1

    writes = []
    lane_power = [rounded[:, j * LANES : (j + 1) * LANES].T for j in range(chunks)]
    for which in range(sets):
        mine = iota((lanes, pixels), 0) // listed == which
        spots = jnp.where(mine, chosen[...].astype(f32), 0.0).astype(bf16)
        taken = covered[which : which + 1, :] > 0.5
        for j in range(chunks):
            cut = slice(j * LANES, (j + 1) * LANES)
            placed = jnp.dot(lane_power[j], spots, preferred_element_type=f32)
            result[which, cut, :] = jnp.where(
                taken, placed, beams[which, cut, :].astype(f32)
            ).astype(bf16)
        copy = pltpu.make_async_copy(
            result.at[which], power.at[which // ranges, which % ranges], out_sem.at[which]
        )
        copy.start()
        writes.append(copy)
    for copy in writes:
        copy.wait()


def slab(n_az, n_acq, image_stack, steering, wiener_filter, range_group, lay_list, lay_count):
    n = n_az * n_acq
    halves, share, azb_all, ranges, pixels = image_stack.shape
    blocks = azb_all // n
    acqs, elevation = steering.shape[2:]
    rows = halves * acqs
    wide = ranges * rows
    sets = blocks * ranges
    lanes = sets * lay_list.shape[2]
    spread = rows * sets
    bf16 = jnp.bfloat16
    f32 = jnp.float32
    vmem = pl.BlockSpec(memory_space=pltpu.VMEM)
    anywhere = pl.BlockSpec(memory_space=pl.ANY)
    ready = pl.pallas_call(
        functools.partial(exchange_kernel, n_az, n_acq),
        out_shape=[
            pltpu.VMEM((halves, acqs, blocks, ranges, pixels), bf16),
            pltpu.VMEM((wide, 2 * elevation), bf16),
            pltpu.VMEM((2 * elevation, wide), bf16),
            pltpu.VMEM((spread, spread), bf16),
            pltpu.VMEM((lanes, pixels), bf16),
            pltpu.VMEM((lanes, wide), f32),
            pltpu.VMEM((sets, pixels), f32),
            pltpu.VMEM((spread, wide), bf16),
        ],
        in_specs=[anywhere] * 6,
        out_specs=[vmem] * 8,
        scratch_shapes=[
            pltpu.SMEM(range_group.shape, jnp.int32),
            pltpu.SMEM(lay_count.shape, jnp.int32),
            pltpu.VMEM(steering.shape, bf16),
            pltpu.VMEM(wiener_filter.shape, bf16),
            pltpu.VMEM(lay_list.shape, jnp.int32),
            pltpu.SemaphoreType.DMA((n,)),
            pltpu.SemaphoreType.DMA((n,)),
            pltpu.SemaphoreType.DMA((6,)),
        ],
        compiler_params=pltpu.CompilerParams(
            collective_id=0, has_side_effects=True
        ),
        name="exchange",
    )(range_group, lay_count, image_stack, steering, wiener_filter, lay_list)
    return pl.pallas_call(
        functools.partial(solve_kernel, ranges),
        out_shape=jax.ShapeDtypeStruct((blocks, ranges, elevation, pixels), bf16),
        in_specs=[vmem] * 8,
        out_specs=anywhere,
        scratch_shapes=[
            pltpu.VMEM((lanes, 2 * elevation), f32),
            pltpu.VMEM((lanes, 2 * elevation), bf16),
            pltpu.VMEM((sets, elevation, pixels), bf16),
            pltpu.VMEM((sets, elevation, pixels), bf16),
            pltpu.SemaphoreType.DMA((sets,)),
        ],
        compiler_params=pltpu.CompilerParams(vmem_limit_bytes=VMEM_LIMIT),
        name="solve",
    )(*[pltpu.with_memory_space_constraint(array, pltpu.VMEM) for array in ready])


def solution(mesh):
    return jax.shard_map(
        functools.partial(slab, mesh.shape["az"], mesh.shape["acq"]),
        mesh=mesh,
        in_specs=(
            P(None, ("az", "acq"), "groups", "rg", None),
            P("rg", None, None, None),
            P("rg", None, None, None),
            P("rg"),
            P(("groups", "az", "acq"), "rg", None),
            P(("groups", "az", "acq"), "rg"),
        ),
        out_specs=P(("groups", "az", "acq"), "rg", None, None),
        check_vma=False,
    )
```

```python
import functools

import jax
import jax.numpy as jnp
from jax import lax
from jax.experimental import pallas as pl
from jax.experimental.pallas import tpu as pltpu
from jax.sharding import PartitionSpec as P

ITERS = 8
STEP_SIZE = 0.5
SHRINK = 0.25
LANES = 128
VMEM_LIMIT = 16 * 1024 * 1024
MESH = pl.DeviceIdType.MESH


def iota(shape, axis):
    return lax.broadcasted_iota(jnp.int32, shape, axis)


def exchange_kernel(
    n_az,
    n_acq,
    range_group_in,
    lay_count_in,
    image,
    steering_in,
    wiener_filter_in,
    lay_list_in,
    recv,
    op,
    op_t,
    gram,
    mix,
    chosen,
    covered,
    gather,
    range_group,
    lay_count,
    steering,
    wiener_filter,
    lay_list,
    send_sem,
    recv_sem,
    ready,
    local_sem,
):
    n = n_az * n_acq
    me = lax.axis_index("az") * n_acq + lax.axis_index("acq")
    halves, share, azb_all, ranges, pixels = image.shape
    blocks = azb_all // n
    groups, _, acqs, elevation = steering.shape
    rows = halves * acqs
    listed = lay_list.shape[2]
    sets = blocks * ranges
    spread = rows * sets
    chunks = elevation // LANES
    bf16 = jnp.bfloat16
    f32 = jnp.float32

    def peer(index):
        return {"az": index // n_acq, "acq": index % n_acq}

    barrier = pltpu.get_barrier_semaphore()
    for other in range(1, n):

        @pl.when(other > me)
        def _():
            pl.semaphore_signal(barrier, inc=1, device_id=peer(other), device_id_type=MESH)

    inputs = []
    for at, (source, target) in enumerate(
        (
            (range_group_in, range_group),
            (lay_count_in, lay_count),
            (steering_in, steering),
            (wiener_filter_in, wiener_filter),
            (lay_list_in, lay_list),
        )
    ):
        copy = pltpu.make_async_copy(source, target, local_sem.at[at + 1])
        copy.start()
        inputs.append(copy)
    local = pltpu.make_async_copy(
        image.at[:, :, pl.ds(blocks * me, blocks)],
        recv.at[:, pl.ds(share * me, share)],
        local_sem.at[0],
    )
    local.start()

    def outgoing(b, there):
        return pltpu.make_async_remote_copy(
            src_ref=image.at[:, :, pl.ds(blocks * there, blocks)],
            dst_ref=recv.at[:, pl.ds(share * me, share)],
            send_sem=send_sem.at[b, there],
            recv_sem=recv_sem.at[b, me],
            device_id=peer(there),
            device_id_type=MESH,
        )

    def incoming(b, source):
        return pltpu.make_async_remote_copy(
            src_ref=image.at[:, :, pl.ds(blocks * me, blocks)],
            dst_ref=recv.at[:, pl.ds(share * source, share)],
            send_sem=send_sem.at[b, source],
            recv_sem=recv_sem.at[b, source],
            device_id=peer(source),
            device_id_type=MESH,
        )

    @pl.when(me > 0)
    def _():
        pl.semaphore_wait(barrier, me)

    for other in range(n - 1):

        @pl.when(other < me)
        def _():
            pl.semaphore_signal(ready.at[me], inc=1, device_id=peer(other), device_id_type=MESH)

    for b in range(1):
        for other in range(n - 1):

            @pl.when(other < me)
            def _():
                outgoing(b, other).start()

    for b in range(1):
        for other in range(1, n):

            @pl.when(other > me)
            def _():
                if b == 0:
                    pl.semaphore_wait(ready.at[other], 1)
                outgoing(b, other).start()

    copy_rows = (iota((rows, spread), 1) // sets == iota((rows, spread), 0)).astype(bf16)
    gather[...] = (iota((spread, rows), 0) // sets == iota((spread, rows), 1)).astype(bf16)
    for copy in inputs:
        copy.wait()
    first_group = lax.axis_index("rg") * groups
    for r in range(ranges):
        group = range_group[r] - first_group
        steer = steering[0]
        filt = wiener_filter[0]
        for g in range(1, groups):
            steer = jnp.where(group == g, steering[g], steer)
            filt = jnp.where(group == g, wiener_filter[g], filt)
        re, im = steer[0], steer[1]
        for j in range(chunks):
            cut = slice(j * LANES, (j + 1) * LANES)
            left = slice(2 * j * LANES, (2 * j + 1) * LANES)
            right = slice((2 * j + 1) * LANES, (2 * j + 2) * LANES)
            op[r, :acqs, left] = re[:, cut]
            op[r, :acqs, right] = -im[:, cut]
            op[r, acqs:, left] = im[:, cut]
            op[r, acqs:, right] = re[:, cut]
        upper = jnp.concatenate([filt[0], -filt[1]], axis=1)
        lower = jnp.concatenate([filt[1], filt[0]], axis=1)
        filter_matrix = jnp.concatenate([upper, lower], axis=0)
        repeated = jnp.dot(filter_matrix, copy_rows, preferred_element_type=f32)
        for b in range(blocks):
            keep = lax.rem(iota((rows, spread), 1), sets) == b * ranges + r
            at = (b * ranges + r) * rows
            mix[at : at + rows, :] = jnp.where(keep, repeated, 0.0).astype(bf16)
        for j in range(2 * chunks):
            op_t[r, j * LANES : (j + 1) * LANES, :] = op[r, :, j * LANES : (j + 1) * LANES].T
        for j in range(chunks):
            left = op_t[r, 2 * j * LANES : (2 * j + 1) * LANES, :]
            part = jnp.dot(left, op[r], preferred_element_type=f32)
            gram[r, j * LANES : (j + 1) * LANES, :] = (-STEP_SIZE * part).astype(bf16)

    diagonal = iota((listed, listed), 0) == iota((listed, listed), 1)
    for b in range(blocks):
        for r in range(ranges):
            entries = lay_list[b, r : r + 1, :].astype(f32)
            column = jnp.sum(jnp.where(diagonal, entries, 0.0), axis=1, keepdims=True)
            alive = iota((listed, pixels), 0) < lay_count[b, r]
            hit = (iota((listed, pixels), 1).astype(f32) == column) & alive
            hot = jnp.where(hit, 1.0, 0.0)
            at = r * blocks + b
            chosen[at * listed : (at + 1) * listed, :] = hot.astype(bf16)
            at = b * ranges + r
            covered[at : at + 1, :] = jnp.sum(hot, axis=0, keepdims=True)

    local.wait()
    for b in range(1):
        for other in range(n):

            @pl.when(other != me)
            def _():
                incoming(b, other).wait_recv()
                outgoing(b, other).wait_send()


def solve_kernel(
    blocks,
    recv,
    op,
    op_t,
    gram,
    mix,
    chosen,
    covered,
    gather,
    power,
    start,
    estimate,
    rounded,
    beams,
    result,
    out_sem,
):
    ranges, rows, wide = op.shape
    spread = mix.shape[0]
    sets = spread // rows
    chunks = wide // (2 * LANES)
    lanes, pixels = chosen.shape
    listed = lanes // sets
    group = lanes // ranges
    bf16 = jnp.bfloat16
    f32 = jnp.float32

    data = recv[...].reshape(spread, pixels)
    picked = lax.dot_general(
        chosen[...], data, (((1,), (1,)), ((), ())), preferred_element_type=f32
    )
    lane, column = iota((lanes, spread), 0), lax.rem(iota((lanes, spread), 1), sets)
    lane_set = lax.rem(lane // listed, blocks) * ranges + lane // group
    target = jnp.dot(
        jnp.where(lane_set == column, picked, 0.0).astype(bf16),
        gather[...],
        preferred_element_type=f32,
    )
    target = (target * (STEP_SIZE / SHRINK)).astype(bf16)
    filtered = [
        jnp.dot(
            mix[which * rows : (which + 1) * rows, :], data, preferred_element_type=f32
        ).astype(bf16)
        for which in range(sets)
    ]

    def beam_unit(unit):
        which, j = divmod(unit, chunks)
        beam = jnp.dot(
            op_t[which % ranges, 2 * j * LANES : (2 * j + 2) * LANES, :],
            filtered[which],
            preferred_element_type=f32,
        )
        re, im = beam[:LANES], beam[LANES:]
        beams[which, j * LANES : (j + 1) * LANES, :] = (re * re + im * im).astype(bf16)

    units = list(range(sets * chunks))
    turns = ITERS * chunks * ranges
    turned = 0
    done = 0
    for turn in range(ITERS):
        for r in range(ranges):
            old = rounded[(turn + 1) % 2, r] if turn > 0 else None
            for j in range(chunks):
                left = slice(2 * j * LANES, (2 * j + 1) * LANES)
                right = slice((2 * j + 1) * LANES, (2 * j + 2) * LANES)
                both = slice(2 * j * LANES, (2 * j + 2) * LANES)
                cut = slice(j * LANES, (j + 1) * LANES)
                if turn == 0:
                    step = jnp.dot(
                        target[r * group : (r + 1) * group],
                        op[r, :, both],
                        preferred_element_type=f32,
                    )
                    z_re, z_im = step[:, :LANES], step[:, LANES:]
                    start[r, :, left] = z_re
                    start[r, :, right] = z_im
                else:
                    step = jnp.dot(old, gram[r, :, both], preferred_element_type=f32)
                    z_re = estimate[r, :, left] + (step[:group, :LANES] - step[group:, LANES:])
                    z_im = estimate[r, :, right] + (step[:group, LANES:] + step[group:, :LANES])
                magnitude = z_re * z_re + z_im * z_im
                factor = jnp.maximum(1.0 - lax.rsqrt(jnp.maximum(magnitude, 1.0)), 0.0)
                x_re, x_im = z_re * factor, z_im * factor
                if turn < ITERS - 1:
                    estimate[r, :, left] = x_re + start[r, :, left]
                    estimate[r, :, right] = x_im + start[r, :, right]
                    rounded[turn % 2, r, :group, cut] = x_re.astype(bf16)
                    rounded[turn % 2, r, group:, cut] = x_im.astype(bf16)
                else:
                    level = (x_re * x_re + x_im * x_im) * (SHRINK * SHRINK)
                    rounded[turn % 2, r, :group, cut] = level.astype(bf16)
                turned += 1
                due = turned * len(units) // turns
                while done < due:
                    beam_unit(units[done])
                    done += 1

    last = (ITERS - 1) % 2
    writes = []
    for r in range(ranges):
        lane_power = [
            rounded[last, r, :group, j * LANES : (j + 1) * LANES].T for j in range(chunks)
        ]
        for b in range(blocks):
            which = b * ranges + r
            mine = iota((group, pixels), 0) // listed == b
            spots = chosen[r * group : (r + 1) * group, :].astype(f32)
            spots = jnp.where(mine, spots, 0.0).astype(bf16)
            taken = covered[which : which + 1, :] > 0.5
            for j in range(chunks):
                cut = slice(j * LANES, (j + 1) * LANES)
                placed = jnp.dot(lane_power[j], spots, preferred_element_type=f32)
                result[which, cut, :] = jnp.where(
                    taken, placed, beams[which, cut, :].astype(f32)
                ).astype(bf16)
            copy = pltpu.make_async_copy(result.at[which], power.at[b, r], out_sem.at[which])
            copy.start()
            writes.append(copy)
    for copy in writes:
        copy.wait()


def slab(n_az, n_acq, image_stack, steering, wiener_filter, range_group, lay_list, lay_count):
    n = n_az * n_acq
    halves, share, azb_all, ranges, pixels = image_stack.shape
    blocks = azb_all // n
    acqs, elevation = steering.shape[2:]
    rows = halves * acqs
    wide = 2 * elevation
    sets = blocks * ranges
    lanes = sets * lay_list.shape[2]
    spread = rows * sets
    bf16 = jnp.bfloat16
    f32 = jnp.float32
    vmem = pl.BlockSpec(memory_space=pltpu.VMEM)
    anywhere = pl.BlockSpec(memory_space=pl.ANY)
    ready = pl.pallas_call(
        functools.partial(exchange_kernel, n_az, n_acq),
        out_shape=[
            pltpu.VMEM((halves, acqs, blocks, ranges, pixels), bf16),
            pltpu.VMEM((ranges, rows, wide), bf16),
            pltpu.VMEM((ranges, wide, rows), bf16),
            pltpu.VMEM((ranges, elevation, wide), bf16),
            pltpu.VMEM((spread, spread), bf16),
            pltpu.VMEM((lanes, pixels), bf16),
            pltpu.VMEM((sets, pixels), f32),
            pltpu.VMEM((spread, rows), bf16),
        ],
        in_specs=[pl.BlockSpec(memory_space=pltpu.HBM)] * 6,
        out_specs=[vmem] * 8,
        scratch_shapes=[
            pltpu.SMEM(range_group.shape, jnp.int32),
            pltpu.SMEM(lay_count.shape, jnp.int32),
            pltpu.VMEM(steering.shape, bf16),
            pltpu.VMEM(wiener_filter.shape, bf16),
            pltpu.VMEM(lay_list.shape, jnp.int32),
            pltpu.SemaphoreType.DMA((blocks, n)),
            pltpu.SemaphoreType.DMA((blocks, n)),
            pltpu.SemaphoreType.REGULAR((n,)),
            pltpu.SemaphoreType.DMA((6,)),
        ],
        compiler_params=pltpu.CompilerParams(
            collective_id=0, has_side_effects=True, vmem_limit_bytes=VMEM_LIMIT
        ),
        name="exchange",
    )(range_group, lay_count, image_stack, steering, wiener_filter, lay_list)
    return pl.pallas_call(
        functools.partial(solve_kernel, blocks),
        out_shape=jax.ShapeDtypeStruct((blocks, ranges, elevation, pixels), bf16),
        in_specs=[vmem] * 8,
        out_specs=anywhere,
        scratch_shapes=[
            pltpu.VMEM((ranges, lanes // ranges, wide), f32),
            pltpu.VMEM((ranges, lanes // ranges, wide), f32),
            pltpu.VMEM((2, ranges, 2 * (lanes // ranges), elevation), bf16),
            pltpu.VMEM((sets, elevation, pixels), bf16),
            pltpu.VMEM((sets, elevation, pixels), bf16),
            pltpu.SemaphoreType.DMA((sets,)),
        ],
        compiler_params=pltpu.CompilerParams(vmem_limit_bytes=VMEM_LIMIT),
        name="solve",
    )(*[pltpu.with_memory_space_constraint(array, pltpu.VMEM) for array in ready])


def solution(mesh):
    return jax.shard_map(
        functools.partial(slab, mesh.shape["az"], mesh.shape["acq"]),
        mesh=mesh,
        in_specs=(
            P(None, ("az", "acq"), "groups", "rg", None),
            P("rg", None, None, None),
            P("rg", None, None, None),
            P("rg"),
            P(("groups", "az", "acq"), "rg", None),
            P(("groups", "az", "acq"), "rg"),
        ),
        out_specs=P(("groups", "az", "acq"), "rg", None, None),
        check_vma=False,
    )
```

```python
import functools

import jax
import jax.numpy as jnp
from jax import lax
from jax.experimental import pallas as pl
from jax.experimental.pallas import tpu as pltpu
from jax.sharding import PartitionSpec as P

ITERS = 8
STEP_SIZE = 0.5
SHRINK = 0.25
LANES = 128
VMEM_LIMIT = 16 * 1024 * 1024
MESH = pl.DeviceIdType.MESH


def iota(shape, axis):
    return lax.broadcasted_iota(jnp.int32, shape, axis)


def exchange_kernel(
    n_az,
    n_acq,
    range_group_in,
    lay_count_in,
    image,
    steering_in,
    wiener_filter_in,
    lay_list_in,
    recv,
    op,
    op_t,
    gram,
    mix,
    chosen,
    covered,
    gather,
    range_group,
    lay_count,
    steering,
    wiener_filter,
    lay_list,
    send_sem,
    recv_sem,
    ready,
    local_sem,
):
    n = n_az * n_acq
    me = lax.axis_index("az") * n_acq + lax.axis_index("acq")
    halves, share, azb_all, ranges, pixels = image.shape
    blocks = azb_all // n
    groups, _, acqs, elevation = steering.shape
    rows = halves * acqs
    listed = lay_list.shape[2]
    sets = blocks * ranges
    spread = rows * sets
    chunks = elevation // LANES
    bf16 = jnp.bfloat16
    f32 = jnp.float32

    def peer(index):
        return {"az": index // n_acq, "acq": index % n_acq}

    barrier = pltpu.get_barrier_semaphore()
    for other in range(1, n):

        @pl.when(other > me)
        def _():
            pl.semaphore_signal(barrier, inc=1, device_id=peer(other), device_id_type=MESH)

    inputs = []
    for at, (source, target) in enumerate(
        (
            (range_group_in, range_group),
            (lay_count_in, lay_count),
            (steering_in, steering),
            (wiener_filter_in, wiener_filter),
            (lay_list_in, lay_list),
        )
    ):
        copy = pltpu.make_async_copy(source, target, local_sem.at[at + 1])
        copy.start()
        inputs.append(copy)
    local = pltpu.make_async_copy(
        image.at[:, :, pl.ds(blocks * me, blocks)],
        recv.at[:, pl.ds(share * me, share)],
        local_sem.at[0],
    )
    local.start()

    def outgoing(b, there):
        return pltpu.make_async_remote_copy(
            src_ref=image.at[:, :, pl.ds(blocks * there, blocks)],
            dst_ref=recv.at[:, pl.ds(share * me, share)],
            send_sem=send_sem.at[b, there],
            recv_sem=recv_sem.at[b, me],
            device_id=peer(there),
            device_id_type=MESH,
        )

    def incoming(b, source):
        return pltpu.make_async_remote_copy(
            src_ref=image.at[:, :, pl.ds(blocks * me, blocks)],
            dst_ref=recv.at[:, pl.ds(share * source, share)],
            send_sem=send_sem.at[b, source],
            recv_sem=recv_sem.at[b, source],
            device_id=peer(source),
            device_id_type=MESH,
        )

    @pl.when(me > 0)
    def _():
        pl.semaphore_wait(barrier, me)

    for other in range(n - 1):

        @pl.when(other < me)
        def _():
            pl.semaphore_signal(ready.at[me], inc=1, device_id=peer(other), device_id_type=MESH)

    for b in range(1):
        for other in range(n - 1):

            @pl.when(other < me)
            def _():
                outgoing(b, other).start()

    for b in range(1):
        for other in range(1, n):

            @pl.when(other > me)
            def _():
                if b == 0:
                    pl.semaphore_wait(ready.at[other], 1)
                outgoing(b, other).start()

    copy_rows = (iota((rows, spread), 1) // sets == iota((rows, spread), 0)).astype(bf16)
    gather[...] = (iota((spread, rows), 0) // sets == iota((spread, rows), 1)).astype(bf16)
    for copy in inputs:
        copy.wait()
    first_group = lax.axis_index("rg") * groups
    for r in range(ranges):
        group = range_group[r] - first_group
        steer = steering[0]
        filt = wiener_filter[0]
        for g in range(1, groups):
            steer = jnp.where(group == g, steering[g], steer)
            filt = jnp.where(group == g, wiener_filter[g], filt)
        re, im = steer[0], steer[1]
        for j in range(chunks):
            cut = slice(j * LANES, (j + 1) * LANES)
            left = slice(2 * j * LANES, (2 * j + 1) * LANES)
            right = slice((2 * j + 1) * LANES, (2 * j + 2) * LANES)
            op[r, :acqs, left] = re[:, cut]
            op[r, :acqs, right] = -im[:, cut]
            op[r, acqs:, left] = im[:, cut]
            op[r, acqs:, right] = re[:, cut]
        upper = jnp.concatenate([filt[0], -filt[1]], axis=1)
        lower = jnp.concatenate([filt[1], filt[0]], axis=1)
        filter_matrix = jnp.concatenate([upper, lower], axis=0)
        repeated = jnp.dot(filter_matrix, copy_rows, preferred_element_type=f32)
        for b in range(blocks):
            keep = lax.rem(iota((rows, spread), 1), sets) == b * ranges + r
            at = (b * ranges + r) * rows
            mix[at : at + rows, :] = jnp.where(keep, repeated, 0.0).astype(bf16)
        for j in range(2 * chunks):
            op_t[r, j * LANES : (j + 1) * LANES, :] = op[r, :, j * LANES : (j + 1) * LANES].T
        for j in range(chunks):
            left = op_t[r, 2 * j * LANES : (2 * j + 1) * LANES, :]
            part = jnp.dot(left, op[r], preferred_element_type=f32)
            gram[r, j * LANES : (j + 1) * LANES, :] = (-STEP_SIZE * part).astype(bf16)

    diagonal = iota((listed, listed), 0) == iota((listed, listed), 1)
    for b in range(blocks):
        for r in range(ranges):
            entries = lay_list[b, r : r + 1, :].astype(f32)
            column = jnp.sum(jnp.where(diagonal, entries, 0.0), axis=1, keepdims=True)
            alive = iota((listed, pixels), 0) < lay_count[b, r]
            hit = (iota((listed, pixels), 1).astype(f32) == column) & alive
            hot = jnp.where(hit, 1.0, 0.0)
            at = r * blocks + b
            chosen[at * listed : (at + 1) * listed, :] = hot.astype(bf16)
            at = b * ranges + r
            covered[at : at + 1, :] = jnp.sum(hot, axis=0, keepdims=True)

    local.wait()
    for b in range(1):
        for other in range(n):

            @pl.when(other != me)
            def _():
                incoming(b, other).wait_recv()
                outgoing(b, other).wait_send()


def solve_kernel(
    blocks,
    recv,
    op,
    op_t,
    gram,
    mix,
    chosen,
    covered,
    gather,
    power,
    start,
    estimate,
    rounded,
    beams,
    result,
    out_sem,
):
    ranges, rows, wide = op.shape
    spread = mix.shape[0]
    sets = spread // rows
    chunks = wide // (2 * LANES)
    lanes, pixels = chosen.shape
    listed = lanes // sets
    group = lanes // ranges
    bf16 = jnp.bfloat16
    f32 = jnp.float32

    data = recv[...].reshape(spread, pixels)
    picked = lax.dot_general(
        chosen[...], data, (((1,), (1,)), ((), ())), preferred_element_type=f32
    )
    lane, column = iota((lanes, spread), 0), lax.rem(iota((lanes, spread), 1), sets)
    lane_set = lax.rem(lane // listed, blocks) * ranges + lane // group
    target = jnp.dot(
        jnp.where(lane_set == column, picked, 0.0).astype(bf16),
        gather[...],
        preferred_element_type=f32,
    )
    target = (target * (STEP_SIZE / SHRINK)).astype(bf16)
    filtered = [
        jnp.dot(
            mix[which * rows : (which + 1) * rows, :], data, preferred_element_type=f32
        ).astype(bf16)
        for which in range(sets)
    ]

    def beam_unit(unit):
        which, j = divmod(unit, chunks)
        beam = jnp.dot(
            op_t[which % ranges, 2 * j * LANES : (2 * j + 2) * LANES, :],
            filtered[which],
            preferred_element_type=f32,
        )
        re, im = beam[:LANES], beam[LANES:]
        beams[which, j * LANES : (j + 1) * LANES, :] = (re * re + im * im).astype(bf16)

    units = list(range(sets * chunks))
    turns = ITERS * chunks * ranges
    turned = 0
    done = 0
    for turn in range(ITERS):
        for r in range(ranges):
            old = rounded[(turn + 1) % 2, r] if turn > 0 else None
            for j in range(chunks):
                left = slice(2 * j * LANES, (2 * j + 1) * LANES)
                right = slice((2 * j + 1) * LANES, (2 * j + 2) * LANES)
                both = slice(2 * j * LANES, (2 * j + 2) * LANES)
                cut = slice(j * LANES, (j + 1) * LANES)
                if turn == 0:
                    step = jnp.dot(
                        target[r * group : (r + 1) * group],
                        op[r, :, both],
                        preferred_element_type=f32,
                    )
                    z_re, z_im = step[:, :LANES], step[:, LANES:]
                    start[r, :, left] = z_re
                    start[r, :, right] = z_im
                else:
                    step = jnp.dot(old, gram[r, :, both], preferred_element_type=f32)
                    z_re = estimate[r, :, left] + (step[:group, :LANES] - step[group:, LANES:])
                    z_im = estimate[r, :, right] + (step[:group, LANES:] + step[group:, :LANES])
                magnitude = z_re * z_re + z_im * z_im
                factor = jnp.maximum(1.0 - lax.rsqrt(jnp.maximum(magnitude, 1.0)), 0.0)
                x_re, x_im = z_re * factor, z_im * factor
                if turn < ITERS - 1:
                    estimate[r, :, left] = x_re + start[r, :, left]
                    estimate[r, :, right] = x_im + start[r, :, right]
                    rounded[turn % 2, r, :group, cut] = x_re.astype(bf16)
                    rounded[turn % 2, r, group:, cut] = x_im.astype(bf16)
                else:
                    level = (x_re * x_re + x_im * x_im) * (SHRINK * SHRINK)
                    rounded[turn % 2, r, :group, cut] = level.astype(bf16)
                turned += 1
                due = turned * len(units) // turns
                while done < due:
                    beam_unit(units[done])
                    done += 1

    last = (ITERS - 1) % 2
    writes = []
    for r in range(ranges):
        lane_power = [
            rounded[last, r, :group, j * LANES : (j + 1) * LANES].T for j in range(chunks)
        ]
        for b in range(blocks):
            which = b * ranges + r
            mine = iota((group, pixels), 0) // listed == b
            spots = chosen[r * group : (r + 1) * group, :].astype(f32)
            spots = jnp.where(mine, spots, 0.0).astype(bf16)
            taken = covered[which : which + 1, :] > 0.5
            for j in range(chunks):
                cut = slice(j * LANES, (j + 1) * LANES)
                placed = jnp.dot(lane_power[j], spots, preferred_element_type=f32)
                result[which, cut, :] = jnp.where(
                    taken, placed, beams[which, cut, :].astype(f32)
                ).astype(bf16)
            copy = pltpu.make_async_copy(result.at[which], power.at[b, r], out_sem.at[which])
            copy.start()
            writes.append(copy)
    for copy in writes:
        copy.wait()


def slab(n_az, n_acq, image_stack, steering, wiener_filter, range_group, lay_list, lay_count):
    n = n_az * n_acq
    halves, share, azb_all, ranges, pixels = image_stack.shape
    blocks = azb_all // n
    acqs, elevation = steering.shape[2:]
    rows = halves * acqs
    wide = 2 * elevation
    sets = blocks * ranges
    lanes = sets * lay_list.shape[2]
    spread = rows * sets
    bf16 = jnp.bfloat16
    f32 = jnp.float32
    vmem = pl.BlockSpec(memory_space=pltpu.VMEM)
    anywhere = pl.BlockSpec(memory_space=pl.ANY)
    ready = pl.pallas_call(
        functools.partial(exchange_kernel, n_az, n_acq),
        out_shape=[
            pltpu.VMEM((halves, acqs, blocks, ranges, pixels), bf16),
            pltpu.VMEM((ranges, rows, wide), bf16),
            pltpu.VMEM((ranges, wide, rows), bf16),
            pltpu.VMEM((ranges, elevation, wide), bf16),
            pltpu.VMEM((spread, spread), bf16),
            pltpu.VMEM((lanes, pixels), bf16),
            pltpu.VMEM((sets, pixels), f32),
            pltpu.VMEM((spread, rows), bf16),
        ],
        in_specs=[pl.BlockSpec(memory_space=pltpu.HBM)] * 6,
        out_specs=[vmem] * 8,
        scratch_shapes=[
            pltpu.SMEM(range_group.shape, jnp.int32),
            pltpu.SMEM(lay_count.shape, jnp.int32),
            pltpu.VMEM(steering.shape, bf16),
            pltpu.VMEM(wiener_filter.shape, bf16),
            pltpu.VMEM(lay_list.shape, jnp.int32),
            pltpu.SemaphoreType.DMA((blocks, n)),
            pltpu.SemaphoreType.DMA((blocks, n)),
            pltpu.SemaphoreType.REGULAR((n,)),
            pltpu.SemaphoreType.DMA((6,)),
        ],
        compiler_params=pltpu.CompilerParams(
            collective_id=0, has_side_effects=True, vmem_limit_bytes=VMEM_LIMIT
        ),
        name="exchange",
    )(*[pltpu.with_memory_space_constraint(array, pltpu.HBM) for array in (range_group, lay_count, image_stack, steering, wiener_filter, lay_list)])
    return pl.pallas_call(
        functools.partial(solve_kernel, blocks),
        out_shape=jax.ShapeDtypeStruct((blocks, ranges, elevation, pixels), bf16),
        in_specs=[vmem] * 8,
        out_specs=anywhere,
        scratch_shapes=[
            pltpu.VMEM((ranges, lanes // ranges, wide), f32),
            pltpu.VMEM((ranges, lanes // ranges, wide), f32),
            pltpu.VMEM((2, ranges, 2 * (lanes // ranges), elevation), bf16),
            pltpu.VMEM((sets, elevation, pixels), bf16),
            pltpu.VMEM((sets, elevation, pixels), bf16),
            pltpu.SemaphoreType.DMA((sets,)),
        ],
        compiler_params=pltpu.CompilerParams(vmem_limit_bytes=VMEM_LIMIT),
        name="solve",
    )(*[pltpu.with_memory_space_constraint(array, pltpu.VMEM) for array in ready])


def solution(mesh):
    return jax.shard_map(
        functools.partial(slab, mesh.shape["az"], mesh.shape["acq"]),
        mesh=mesh,
        in_specs=(
            P(None, ("az", "acq"), "groups", "rg", None),
            P("rg", None, None, None),
            P("rg", None, None, None),
            P("rg"),
            P(("groups", "az", "acq"), "rg", None),
            P(("groups", "az", "acq"), "rg"),
        ),
        out_specs=P(("groups", "az", "acq"), "rg", None, None),
        check_vma=False,
    )
```

```python
import functools

import jax
import jax.numpy as jnp
from jax import lax
from jax.experimental import pallas as pl
from jax.experimental.pallas import tpu as pltpu
from jax.sharding import PartitionSpec as P

ITERS = 8
STEP_SIZE = 0.5
SHRINK = 0.25
LANES = 128
VMEM_LIMIT = 16 * 1024 * 1024
MESH = pl.DeviceIdType.MESH


def iota(shape, axis):
    return lax.broadcasted_iota(jnp.int32, shape, axis)


def exchange_kernel(
    n_az,
    n_acq,
    range_group_in,
    lay_count_in,
    image,
    steering_in,
    wiener_filter_in,
    lay_list_in,
    recv,
    op,
    op_t,
    gram,
    mix,
    chosen,
    covered,
    gather,
    range_group,
    lay_count,
    steering,
    wiener_filter,
    lay_list,
    staged,
    send_sem,
    recv_sem,
    ready,
    gate,
    local_sem,
):
    n = n_az * n_acq
    me = lax.axis_index("az") * n_acq + lax.axis_index("acq")
    halves, share, azb_all, ranges, pixels = image.shape
    blocks = azb_all // n
    groups, _, acqs, elevation = steering.shape
    rows = halves * acqs
    listed = lay_list.shape[2]
    sets = blocks * ranges
    spread = rows * sets
    chunks = elevation // LANES
    bf16 = jnp.bfloat16
    f32 = jnp.float32

    half = n_az // 2 * n_acq

    def peer(index):
        return {"az": index // n_acq, "acq": index % n_acq}

    barrier = pltpu.get_barrier_semaphore()
    for other in range(1, n):

        @pl.when(other > me)
        def _():
            pl.semaphore_signal(barrier, inc=1, device_id=peer(other), device_id_type=MESH)

    inputs = []
    for at, (source, target) in enumerate(
        (
            (range_group_in, range_group),
            (lay_count_in, lay_count),
            (steering_in, steering),
            (wiener_filter_in, wiener_filter),
            (lay_list_in, lay_list),
        )
    ):
        copy = pltpu.make_async_copy(source, target, local_sem.at[at + 1])
        copy.start()
        inputs.append(copy)
    local = pltpu.make_async_copy(
        image.at[:, :, pl.ds(blocks * me, blocks)],
        recv.at[:, pl.ds(share * me, share)],
        local_sem.at[0],
    )
    local.start()

    stage = pltpu.make_async_copy(image, staged, local_sem.at[6])

    @pl.when(me < half)
    def _():
        stage.start()

    def outgoing(b, there, source=image):
        return pltpu.make_async_remote_copy(
            src_ref=source.at[:, :, pl.ds(blocks * there, blocks)],
            dst_ref=recv.at[:, pl.ds(share * me, share)],
            send_sem=send_sem.at[b, there],
            recv_sem=recv_sem.at[b, me],
            device_id=peer(there),
            device_id_type=MESH,
        )

    def incoming(b, source):
        return pltpu.make_async_remote_copy(
            src_ref=image.at[:, :, pl.ds(blocks * me, blocks)],
            dst_ref=recv.at[:, pl.ds(share * source, share)],
            send_sem=send_sem.at[b, source],
            recv_sem=recv_sem.at[b, source],
            device_id=peer(source),
            device_id_type=MESH,
        )

    @pl.when(me > 0)
    def _():
        pl.semaphore_wait(barrier, me)

    for other in range(n - 1):

        @pl.when(other < me)
        def _():
            pl.semaphore_signal(ready.at[me], inc=1, device_id=peer(other), device_id_type=MESH)

    az = me // n_acq
    middle = n_az // 2
    inner = (az >= middle) & (az + 1 < n_az)
    outer = (az > middle) & (az < n_az)

    def held(other):
        return (inner & (other // n_acq == middle - 1)) | (outer & (other >= n_acq))

    for other in range(n - 1):

        @pl.when((other < me) & jnp.logical_not(held(other)))
        def _():
            outgoing(0, other).start()

    @pl.when(me < half)
    def _():
        stage.wait()

    for other in range(1, n):

        @pl.when(other > me)
        def _():
            pl.semaphore_wait(ready.at[other], 1)

        @pl.when((other > me) & (me < half))
        def _():
            outgoing(0, other, staged).start()

        @pl.when((other > me) & (me >= half))
        def _():
            outgoing(0, other).start()

    copy_rows = (iota((rows, spread), 1) // sets == iota((rows, spread), 0)).astype(bf16)
    gather[...] = (iota((spread, rows), 0) // sets == iota((spread, rows), 1)).astype(bf16)
    for copy in inputs:
        copy.wait()
    first_group = lax.axis_index("rg") * groups
    for r in range(ranges):
        group = range_group[r] - first_group
        steer = steering[0]
        filt = wiener_filter[0]
        for g in range(1, groups):
            steer = jnp.where(group == g, steering[g], steer)
            filt = jnp.where(group == g, wiener_filter[g], filt)
        re, im = steer[0], steer[1]
        for j in range(chunks):
            cut = slice(j * LANES, (j + 1) * LANES)
            left = slice(2 * j * LANES, (2 * j + 1) * LANES)
            right = slice((2 * j + 1) * LANES, (2 * j + 2) * LANES)
            op[r, :acqs, left] = re[:, cut]
            op[r, :acqs, right] = -im[:, cut]
            op[r, acqs:, left] = im[:, cut]
            op[r, acqs:, right] = re[:, cut]
        upper = jnp.concatenate([filt[0], -filt[1]], axis=1)
        lower = jnp.concatenate([filt[1], filt[0]], axis=1)
        filter_matrix = jnp.concatenate([upper, lower], axis=0)
        repeated = jnp.dot(filter_matrix, copy_rows, preferred_element_type=f32)
        for b in range(blocks):
            keep = lax.rem(iota((rows, spread), 1), sets) == b * ranges + r
            at = (b * ranges + r) * rows
            mix[at : at + rows, :] = jnp.where(keep, repeated, 0.0).astype(bf16)
        for j in range(2 * chunks):
            op_t[r, j * LANES : (j + 1) * LANES, :] = op[r, :, j * LANES : (j + 1) * LANES].T
        for j in range(chunks):
            left = op_t[r, 2 * j * LANES : (2 * j + 1) * LANES, :]
            part = jnp.dot(left, op[r], preferred_element_type=f32)
            gram[r, j * LANES : (j + 1) * LANES, :] = (-STEP_SIZE * part).astype(bf16)

    diagonal = iota((listed, listed), 0) == iota((listed, listed), 1)
    for b in range(blocks):
        for r in range(ranges):
            entries = lay_list[b, r : r + 1, :].astype(f32)
            column = jnp.sum(jnp.where(diagonal, entries, 0.0), axis=1, keepdims=True)
            alive = iota((listed, pixels), 0) < lay_count[b, r]
            hit = (iota((listed, pixels), 1).astype(f32) == column) & alive
            hot = jnp.where(hit, 1.0, 0.0)
            at = r * blocks + b
            chosen[at * listed : (at + 1) * listed, :] = hot.astype(bf16)
            at = b * ranges + r
            covered[at : at + 1, :] = jnp.sum(hot, axis=0, keepdims=True)

    @pl.when(outer)
    def _():
        for near in range(n_acq):
            outgoing(0, near).wait_send()
        pl.semaphore_signal(gate, inc=1, device_id=peer(me - n_acq), device_id_type=MESH)

    @pl.when(inner)
    def _():
        pl.semaphore_wait(gate, 1)

    for other in range(n - 1):

        @pl.when((other < me) & held(other))
        def _():
            outgoing(0, other).start()

    local.wait()
    for other in range(n):

        @pl.when(other != me)
        def _():
            incoming(0, other).wait_recv()

        @pl.when((other != me) & jnp.logical_not(outer) if other < n_acq else other != me)
        def _():
            outgoing(0, other).wait_send()


def solve_kernel(
    blocks,
    recv,
    op,
    op_t,
    gram,
    mix,
    chosen,
    covered,
    gather,
    power,
    start,
    estimate,
    rounded,
    beams,
    result,
    out_sem,
):
    ranges, rows, wide = op.shape
    spread = mix.shape[0]
    sets = spread // rows
    chunks = wide // (2 * LANES)
    lanes, pixels = chosen.shape
    listed = lanes // sets
    group = lanes // ranges
    bf16 = jnp.bfloat16
    f32 = jnp.float32

    data = recv[...].reshape(spread, pixels)
    picked = lax.dot_general(
        chosen[...], data, (((1,), (1,)), ((), ())), preferred_element_type=f32
    )
    lane, column = iota((lanes, spread), 0), lax.rem(iota((lanes, spread), 1), sets)
    lane_set = lax.rem(lane // listed, blocks) * ranges + lane // group
    target = jnp.dot(
        jnp.where(lane_set == column, picked, 0.0).astype(bf16),
        gather[...],
        preferred_element_type=f32,
    )
    target = (target * (STEP_SIZE / SHRINK)).astype(bf16)
    filtered = [
        jnp.dot(
            mix[which * rows : (which + 1) * rows, :], data, preferred_element_type=f32
        ).astype(bf16)
        for which in range(sets)
    ]

    def beam_unit(unit):
        which, j = divmod(unit, chunks)
        beam = jnp.dot(
            op_t[which % ranges, 2 * j * LANES : (2 * j + 2) * LANES, :],
            filtered[which],
            preferred_element_type=f32,
        )
        re, im = beam[:LANES], beam[LANES:]
        beams[which, j * LANES : (j + 1) * LANES, :] = (re * re + im * im).astype(bf16)

    units = list(range(sets * chunks))
    turns = ITERS * chunks * ranges
    turned = 0
    done = 0
    for turn in range(ITERS):
        for r in range(ranges):
            old = rounded[(turn + 1) % 2, r] if turn > 0 else None
            for j in range(chunks):
                left = slice(2 * j * LANES, (2 * j + 1) * LANES)
                right = slice((2 * j + 1) * LANES, (2 * j + 2) * LANES)
                both = slice(2 * j * LANES, (2 * j + 2) * LANES)
                cut = slice(j * LANES, (j + 1) * LANES)
                if turn == 0:
                    step = jnp.dot(
                        target[r * group : (r + 1) * group],
                        op[r, :, both],
                        preferred_element_type=f32,
                    )
                    z_re, z_im = step[:, :LANES], step[:, LANES:]
                    start[r, :, left] = z_re
                    start[r, :, right] = z_im
                else:
                    step = jnp.dot(old, gram[r, :, both], preferred_element_type=f32)
                    z_re = estimate[r, :, left] + (step[:group, :LANES] - step[group:, LANES:])
                    z_im = estimate[r, :, right] + (step[:group, LANES:] + step[group:, :LANES])
                magnitude = z_re * z_re + z_im * z_im
                factor = jnp.maximum(1.0 - lax.rsqrt(jnp.maximum(magnitude, 1.0)), 0.0)
                x_re, x_im = z_re * factor, z_im * factor
                if turn < ITERS - 1:
                    estimate[r, :, left] = x_re + start[r, :, left]
                    estimate[r, :, right] = x_im + start[r, :, right]
                    rounded[turn % 2, r, :group, cut] = x_re.astype(bf16)
                    rounded[turn % 2, r, group:, cut] = x_im.astype(bf16)
                else:
                    level = (x_re * x_re + x_im * x_im) * (SHRINK * SHRINK)
                    rounded[turn % 2, r, :group, cut] = level.astype(bf16)
                turned += 1
                due = turned * len(units) // turns
                while done < due:
                    beam_unit(units[done])
                    done += 1

    last = (ITERS - 1) % 2
    writes = []
    for r in range(ranges):
        lane_power = [
            rounded[last, r, :group, j * LANES : (j + 1) * LANES].T for j in range(chunks)
        ]
        for b in range(blocks):
            which = b * ranges + r
            mine = iota((group, pixels), 0) // listed == b
            spots = chosen[r * group : (r + 1) * group, :].astype(f32)
            spots = jnp.where(mine, spots, 0.0).astype(bf16)
            taken = covered[which : which + 1, :] > 0.5
            for j in range(chunks):
                cut = slice(j * LANES, (j + 1) * LANES)
                placed = jnp.dot(lane_power[j], spots, preferred_element_type=f32)
                result[which, cut, :] = jnp.where(
                    taken, placed, beams[which, cut, :].astype(f32)
                ).astype(bf16)
            copy = pltpu.make_async_copy(result.at[which], power.at[b, r], out_sem.at[which])
            copy.start()
            writes.append(copy)
    for copy in writes:
        copy.wait()


def slab(n_az, n_acq, image_stack, steering, wiener_filter, range_group, lay_list, lay_count):
    n = n_az * n_acq
    halves, share, azb_all, ranges, pixels = image_stack.shape
    blocks = azb_all // n
    acqs, elevation = steering.shape[2:]
    rows = halves * acqs
    wide = 2 * elevation
    sets = blocks * ranges
    lanes = sets * lay_list.shape[2]
    spread = rows * sets
    bf16 = jnp.bfloat16
    f32 = jnp.float32
    vmem = pl.BlockSpec(memory_space=pltpu.VMEM)
    anywhere = pl.BlockSpec(memory_space=pl.ANY)
    ready = pl.pallas_call(
        functools.partial(exchange_kernel, n_az, n_acq),
        out_shape=[
            pltpu.VMEM((halves, acqs, blocks, ranges, pixels), bf16),
            pltpu.VMEM((ranges, rows, wide), bf16),
            pltpu.VMEM((ranges, wide, rows), bf16),
            pltpu.VMEM((ranges, elevation, wide), bf16),
            pltpu.VMEM((spread, spread), bf16),
            pltpu.VMEM((lanes, pixels), bf16),
            pltpu.VMEM((sets, pixels), f32),
            pltpu.VMEM((spread, rows), bf16),
        ],
        in_specs=[pl.BlockSpec(memory_space=pltpu.HBM)] * 6,
        out_specs=[vmem] * 8,
        scratch_shapes=[
            pltpu.SMEM(range_group.shape, jnp.int32),
            pltpu.SMEM(lay_count.shape, jnp.int32),
            pltpu.VMEM(steering.shape, bf16),
            pltpu.VMEM(wiener_filter.shape, bf16),
            pltpu.VMEM(lay_list.shape, jnp.int32),
            pltpu.VMEM(image_stack.shape, bf16),
            pltpu.SemaphoreType.DMA((blocks, n)),
            pltpu.SemaphoreType.DMA((blocks, n)),
            pltpu.SemaphoreType.REGULAR((n,)),
            pltpu.SemaphoreType.REGULAR,
            pltpu.SemaphoreType.DMA((7,)),
        ],
        compiler_params=pltpu.CompilerParams(
            collective_id=0, has_side_effects=True, vmem_limit_bytes=VMEM_LIMIT
        ),
        name="exchange",
    )(*[pltpu.with_memory_space_constraint(array, pltpu.HBM) for array in (range_group, lay_count, image_stack, steering, wiener_filter, lay_list)])
    return pl.pallas_call(
        functools.partial(solve_kernel, blocks),
        out_shape=jax.ShapeDtypeStruct((blocks, ranges, elevation, pixels), bf16),
        in_specs=[vmem] * 8,
        out_specs=anywhere,
        scratch_shapes=[
            pltpu.VMEM((ranges, lanes // ranges, wide), f32),
            pltpu.VMEM((ranges, lanes // ranges, wide), f32),
            pltpu.VMEM((2, ranges, 2 * (lanes // ranges), elevation), bf16),
            pltpu.VMEM((sets, elevation, pixels), bf16),
            pltpu.VMEM((sets, elevation, pixels), bf16),
            pltpu.SemaphoreType.DMA((sets,)),
        ],
        compiler_params=pltpu.CompilerParams(vmem_limit_bytes=VMEM_LIMIT),
        name="solve",
    )(*[pltpu.with_memory_space_constraint(array, pltpu.VMEM) for array in ready])


def solution(mesh):
    return jax.shard_map(
        functools.partial(slab, mesh.shape["az"], mesh.shape["acq"]),
        mesh=mesh,
        in_specs=(
            P(None, ("az", "acq"), "groups", "rg", None),
            P("rg", None, None, None),
            P("rg", None, None, None),
            P("rg"),
            P(("groups", "az", "acq"), "rg", None),
            P(("groups", "az", "acq"), "rg"),
        ),
        out_specs=P(("groups", "az", "acq"), "rg", None, None),
        check_vma=False,
    )
```

```python
import functools

import jax
import jax.numpy as jnp
from jax import lax
from jax.experimental import pallas as pl
from jax.experimental.pallas import tpu as pltpu
from jax.sharding import PartitionSpec as P

ITERS = 8
STEP_SIZE = 0.5
SHRINK = 0.25
LANES = 128
VMEM_LIMIT = 16 * 1024 * 1024
MESH = pl.DeviceIdType.MESH


def iota(shape, axis):
    return lax.broadcasted_iota(jnp.int32, shape, axis)


def exchange_kernel(
    n_az,
    n_acq,
    range_group_in,
    lay_count_in,
    image,
    steering_in,
    wiener_filter_in,
    lay_list_in,
    recv,
    op,
    op_t,
    gram,
    mix,
    chosen,
    covered,
    gather,
    range_group,
    lay_count,
    steering,
    wiener_filter,
    lay_list,
    staged,
    send_sem,
    recv_sem,
    ready,
    gate,
    local_sem,
):
    n = n_az * n_acq
    me = lax.axis_index("az") * n_acq + lax.axis_index("acq")
    halves, share, azb_all, ranges, pixels = image.shape
    blocks = azb_all // n
    groups, _, acqs, elevation = steering.shape
    rows = halves * acqs
    listed = lay_list.shape[2]
    sets = blocks * ranges
    spread = rows * sets
    chunks = elevation // LANES
    bf16 = jnp.bfloat16
    f32 = jnp.float32

    half = n_az // 2 * n_acq

    def peer(index):
        return {"az": index // n_acq, "acq": index % n_acq}

    barrier = pltpu.get_barrier_semaphore()
    for other in range(1, n):

        @pl.when(other > me)
        def _():
            pl.semaphore_signal(barrier, inc=1, device_id=peer(other), device_id_type=MESH)

    inputs = []
    for at, (source, target) in enumerate(
        (
            (range_group_in, range_group),
            (lay_count_in, lay_count),
            (steering_in, steering),
            (wiener_filter_in, wiener_filter),
            (lay_list_in, lay_list),
        )
    ):
        copy = pltpu.make_async_copy(source, target, local_sem.at[at + 1])
        copy.start()
        inputs.append(copy)
    local = pltpu.make_async_copy(
        image.at[:, :, pl.ds(blocks * me, blocks)],
        recv.at[:, pl.ds(share * me, share)],
        local_sem.at[0],
    )
    local.start()

    stage = pltpu.make_async_copy(image, staged, local_sem.at[6])

    @pl.when(me < half)
    def _():
        stage.start()

    def outgoing(b, there, source=image):
        return pltpu.make_async_remote_copy(
            src_ref=source.at[:, :, pl.ds(blocks * there, blocks)],
            dst_ref=recv.at[:, pl.ds(share * me, share)],
            send_sem=send_sem.at[b, there],
            recv_sem=recv_sem.at[b, me],
            device_id=peer(there),
            device_id_type=MESH,
        )

    def incoming(b, source):
        return pltpu.make_async_remote_copy(
            src_ref=image.at[:, :, pl.ds(blocks * me, blocks)],
            dst_ref=recv.at[:, pl.ds(share * source, share)],
            send_sem=send_sem.at[b, source],
            recv_sem=recv_sem.at[b, source],
            device_id=peer(source),
            device_id_type=MESH,
        )

    @pl.when(me > 0)
    def _():
        pl.semaphore_wait(barrier, me)

    for other in range(n - 1):

        @pl.when(other < me)
        def _():
            pl.semaphore_signal(ready.at[me], inc=1, device_id=peer(other), device_id_type=MESH)

    az = me // n_acq
    middle = n_az // 2
    inner = (az >= middle) & (az + 1 < n_az)
    outer = (az > middle) & (az < n_az)

    def held(other):
        return (inner & (other // n_acq == middle - 1)) | (outer & (other >= n_acq))

    for other in range(n - 1):

        @pl.when((other < me) & jnp.logical_not(held(other)))
        def _():
            outgoing(0, other).start()

    @pl.when(me < half)
    def _():
        stage.wait()

    for other in range(1, n):

        @pl.when(other > me)
        def _():
            pl.semaphore_wait(ready.at[other], 1)

        @pl.when((other > me) & (me < half))
        def _():
            outgoing(0, other, staged).start()

        @pl.when((other > me) & (me >= half))
        def _():
            outgoing(0, other).start()

    copy_rows = (iota((rows, spread), 1) // sets == iota((rows, spread), 0)).astype(bf16)
    gather[...] = (iota((spread, rows), 0) // sets == iota((spread, rows), 1)).astype(bf16)
    for copy in inputs:
        copy.wait()
    first_group = lax.axis_index("rg") * groups
    for r in range(ranges):
        group = range_group[r] - first_group
        steer = steering[0]
        filt = wiener_filter[0]
        for g in range(1, groups):
            steer = jnp.where(group == g, steering[g], steer)
            filt = jnp.where(group == g, wiener_filter[g], filt)
        re, im = steer[0], steer[1]
        for j in range(chunks):
            cut = slice(j * LANES, (j + 1) * LANES)
            left = slice(2 * j * LANES, (2 * j + 1) * LANES)
            right = slice((2 * j + 1) * LANES, (2 * j + 2) * LANES)
            op[r, :acqs, left] = re[:, cut]
            op[r, :acqs, right] = -im[:, cut]
            op[r, acqs:, left] = im[:, cut]
            op[r, acqs:, right] = re[:, cut]
        upper = jnp.concatenate([filt[0], -filt[1]], axis=1)
        lower = jnp.concatenate([filt[1], filt[0]], axis=1)
        filter_matrix = jnp.concatenate([upper, lower], axis=0)
        repeated = jnp.dot(filter_matrix, copy_rows, preferred_element_type=f32)
        for b in range(blocks):
            keep = lax.rem(iota((rows, spread), 1), sets) == b * ranges + r
            at = (b * ranges + r) * rows
            mix[at : at + rows, :] = jnp.where(keep, repeated, 0.0).astype(bf16)
        for j in range(2 * chunks):
            op_t[r, j * LANES : (j + 1) * LANES, :] = op[r, :, j * LANES : (j + 1) * LANES].T
        for j in range(chunks):
            left = op_t[r, 2 * j * LANES : (2 * j + 1) * LANES, :]
            part = jnp.dot(left, op[r], preferred_element_type=f32)
            gram[r, j * LANES : (j + 1) * LANES, :] = (-STEP_SIZE * part).astype(bf16)

    diagonal = iota((listed, listed), 0) == iota((listed, listed), 1)
    for b in range(blocks):
        for r in range(ranges):
            entries = lay_list[b, r : r + 1, :].astype(f32)
            column = jnp.sum(jnp.where(diagonal, entries, 0.0), axis=1, keepdims=True)
            alive = iota((listed, pixels), 0) < lay_count[b, r]
            hit = (iota((listed, pixels), 1).astype(f32) == column) & alive
            hot = jnp.where(hit, 1.0, 0.0)
            at = r * blocks + b
            chosen[at * listed : (at + 1) * listed, :] = hot.astype(bf16)
            at = b * ranges + r
            covered[at : at + 1, :] = jnp.sum(hot, axis=0, keepdims=True)

    @pl.when(outer)
    def _():
        for near in range(n_acq):
            outgoing(0, near).wait_send()
        pl.semaphore_signal(gate, inc=1, device_id=peer(me - n_acq), device_id_type=MESH)

    @pl.when(inner)
    def _():
        pl.semaphore_wait(gate, 1)

    for other in range(n - 1):

        @pl.when((other < me) & held(other))
        def _():
            outgoing(0, other).start()

    local.wait()
    for other in range(n):

        @pl.when(other != me)
        def _():
            incoming(0, other).wait_recv()

        @pl.when((other != me) & jnp.logical_not(outer) if other < n_acq else other != me)
        def _():
            outgoing(0, other).wait_send()


def solve_kernel(
    blocks,
    recv,
    op,
    op_t,
    gram,
    mix,
    chosen,
    covered,
    gather,
    power,
    start,
    estimate,
    rounded,
    beams,
    result,
    out_sem,
):
    ranges, rows, wide = op.shape
    spread = mix.shape[0]
    sets = spread // rows
    chunks = wide // (2 * LANES)
    lanes, pixels = chosen.shape
    listed = lanes // sets
    group = lanes // ranges
    bf16 = jnp.bfloat16
    f32 = jnp.float32

    data = recv[...].reshape(spread, pixels)
    picked = lax.dot_general(
        chosen[...], data, (((1,), (1,)), ((), ())), preferred_element_type=f32
    )
    lane, column = iota((lanes, spread), 0), lax.rem(iota((lanes, spread), 1), sets)
    lane_set = lax.rem(lane // listed, blocks) * ranges + lane // group
    target = jnp.dot(
        jnp.where(lane_set == column, picked, 0.0).astype(bf16),
        gather[...],
        preferred_element_type=f32,
    )
    target = (target * (STEP_SIZE / SHRINK)).astype(bf16)
    filtered = []
    for which in range(sets):
        product = jnp.dot(
            mix[which * rows : (which + 1) * rows, :], data, preferred_element_type=f32
        )
        taken = covered[which : which + 1, :] > 0.5
        filtered.append(jnp.where(taken, 0.0, product).astype(bf16))

    def beam_unit(unit):
        which, j = divmod(unit, chunks)
        beam = jnp.dot(
            op_t[which % ranges, 2 * j * LANES : (2 * j + 2) * LANES, :],
            filtered[which],
            preferred_element_type=f32,
        )
        re, im = beam[:LANES], beam[LANES:]
        beams[which, j * LANES : (j + 1) * LANES, :] = (re * re + im * im).astype(bf16)

    units = list(range(sets * chunks))
    turns = ITERS * chunks * ranges
    turned = 0
    done = 0
    for turn in range(ITERS):
        for r in range(ranges):
            old = rounded[(turn + 1) % 2, r] if turn > 0 else None
            for j in range(chunks):
                left = slice(2 * j * LANES, (2 * j + 1) * LANES)
                right = slice((2 * j + 1) * LANES, (2 * j + 2) * LANES)
                both = slice(2 * j * LANES, (2 * j + 2) * LANES)
                cut = slice(j * LANES, (j + 1) * LANES)
                if turn == 0:
                    step = jnp.dot(
                        target[r * group : (r + 1) * group],
                        op[r, :, both],
                        preferred_element_type=f32,
                    )
                    z_re, z_im = step[:, :LANES], step[:, LANES:]
                    start[r, :, left] = z_re
                    start[r, :, right] = z_im
                else:
                    mid = wide // 4
                    step = jnp.dot(old[:, :mid], gram[r, :mid, both], preferred_element_type=f32)
                    step = step + jnp.dot(old[:, mid:], gram[r, mid:, both], preferred_element_type=f32)
                    z_re = estimate[r, :, left] + (step[:group, :LANES] - step[group:, LANES:])
                    z_im = estimate[r, :, right] + (step[:group, LANES:] + step[group:, :LANES])
                magnitude = z_re * z_re + z_im * z_im
                factor = jnp.maximum(1.0 - lax.rsqrt(jnp.maximum(magnitude, 1.0)), 0.0)
                x_re, x_im = z_re * factor, z_im * factor
                if turn < ITERS - 1:
                    estimate[r, :, left] = x_re + start[r, :, left]
                    estimate[r, :, right] = x_im + start[r, :, right]
                    rounded[turn % 2, r, :group, cut] = x_re.astype(bf16)
                    rounded[turn % 2, r, group:, cut] = x_im.astype(bf16)
                else:
                    level = (x_re * x_re + x_im * x_im) * (SHRINK * SHRINK)
                    rounded[turn % 2, r, :group, cut] = level.astype(bf16)
                turned += 1
                due = turned * len(units) // turns
                while done < due:
                    beam_unit(units[done])
                    done += 1

    last = (ITERS - 1) % 2
    writes = []
    for r in range(ranges):
        lane_power = [
            rounded[last, r, :group, j * LANES : (j + 1) * LANES].T for j in range(chunks)
        ]
        for b in range(blocks):
            which = b * ranges + r
            mine = iota((group, pixels), 0) // listed == b
            spots = chosen[r * group : (r + 1) * group, :].astype(f32)
            spots = jnp.where(mine, spots, 0.0).astype(bf16)
            for j in range(chunks):
                cut = slice(j * LANES, (j + 1) * LANES)
                placed = jnp.dot(lane_power[j], spots, preferred_element_type=f32)
                result[which, cut, :] = (beams[which, cut, :].astype(f32) + placed).astype(bf16)
            copy = pltpu.make_async_copy(result.at[which], power.at[b, r], out_sem.at[which])
            copy.start()
            writes.append(copy)
    for copy in writes:
        copy.wait()


def slab(n_az, n_acq, image_stack, steering, wiener_filter, range_group, lay_list, lay_count):
    n = n_az * n_acq
    halves, share, azb_all, ranges, pixels = image_stack.shape
    blocks = azb_all // n
    acqs, elevation = steering.shape[2:]
    rows = halves * acqs
    wide = 2 * elevation
    sets = blocks * ranges
    lanes = sets * lay_list.shape[2]
    spread = rows * sets
    bf16 = jnp.bfloat16
    f32 = jnp.float32
    vmem = pl.BlockSpec(memory_space=pltpu.VMEM)
    anywhere = pl.BlockSpec(memory_space=pl.ANY)
    ready = pl.pallas_call(
        functools.partial(exchange_kernel, n_az, n_acq),
        out_shape=[
            pltpu.VMEM((halves, acqs, blocks, ranges, pixels), bf16),
            pltpu.VMEM((ranges, rows, wide), bf16),
            pltpu.VMEM((ranges, wide, rows), bf16),
            pltpu.VMEM((ranges, elevation, wide), bf16),
            pltpu.VMEM((spread, spread), bf16),
            pltpu.VMEM((lanes, pixels), bf16),
            pltpu.VMEM((sets, pixels), f32),
            pltpu.VMEM((spread, rows), bf16),
        ],
        in_specs=[pl.BlockSpec(memory_space=pltpu.HBM)] * 6,
        out_specs=[vmem] * 8,
        scratch_shapes=[
            pltpu.SMEM(range_group.shape, jnp.int32),
            pltpu.SMEM(lay_count.shape, jnp.int32),
            pltpu.VMEM(steering.shape, bf16),
            pltpu.VMEM(wiener_filter.shape, bf16),
            pltpu.VMEM(lay_list.shape, jnp.int32),
            pltpu.VMEM(image_stack.shape, bf16),
            pltpu.SemaphoreType.DMA((blocks, n)),
            pltpu.SemaphoreType.DMA((blocks, n)),
            pltpu.SemaphoreType.REGULAR((n,)),
            pltpu.SemaphoreType.REGULAR,
            pltpu.SemaphoreType.DMA((7,)),
        ],
        compiler_params=pltpu.CompilerParams(
            collective_id=0, has_side_effects=True, vmem_limit_bytes=VMEM_LIMIT
        ),
        name="exchange",
    )(*[pltpu.with_memory_space_constraint(array, pltpu.HBM) for array in (range_group, lay_count, image_stack, steering, wiener_filter, lay_list)])
    return pl.pallas_call(
        functools.partial(solve_kernel, blocks),
        out_shape=jax.ShapeDtypeStruct((blocks, ranges, elevation, pixels), bf16),
        in_specs=[vmem] * 8,
        out_specs=anywhere,
        scratch_shapes=[
            pltpu.VMEM((ranges, lanes // ranges, wide), f32),
            pltpu.VMEM((ranges, lanes // ranges, wide), f32),
            pltpu.VMEM((2, ranges, 2 * (lanes // ranges), elevation), bf16),
            pltpu.VMEM((sets, elevation, pixels), bf16),
            pltpu.VMEM((sets, elevation, pixels), bf16),
            pltpu.SemaphoreType.DMA((sets,)),
        ],
        compiler_params=pltpu.CompilerParams(vmem_limit_bytes=VMEM_LIMIT),
        name="solve",
    )(*[pltpu.with_memory_space_constraint(array, pltpu.VMEM) for array in ready])


def solution(mesh):
    return jax.shard_map(
        functools.partial(slab, mesh.shape["az"], mesh.shape["acq"]),
        mesh=mesh,
        in_specs=(
            P(None, ("az", "acq"), "groups", "rg", None),
            P("rg", None, None, None),
            P("rg", None, None, None),
            P("rg"),
            P(("groups", "az", "acq"), "rg", None),
            P(("groups", "az", "acq"), "rg"),
        ),
        out_specs=P(("groups", "az", "acq"), "rg", None, None),
        check_vma=False,
    )
```
